32 devices in a mesh: wide: 8 (over y, x, core), narrow: 4 (over z).
Axes of the slice: x: 2, y: 2, z: 4, core: 2. Of those that a mesh axis runs over, the one named last changes fastest.
Arguments:
- schur_matrix: bfloat16 [8, 4, 3, 1024, 1024], P('wide', 'narrow')
- face_inverse: bfloat16 [8, 4, 3, 8, 128, 128], P('wide', 'narrow')
- deluxe: bfloat16 [8, 4, 3, 8, 128, 128], P('wide', 'narrow')
- primal_weight: float32 [8, 4, 3, 8, 128], P('wide', 'narrow'), may hold values from 0.05 to 0.3
- coarse_group: float32 [8, 96, 96], P('wide', 'narrow')
- coarse_map: float32 [8, 96, 8], P('wide', 'narrow'), may hold values from -0.625 to 0.625
- coarse_top: float32 [64, 64], P('wide')
- load_vector: bfloat16 [8, 4, 3, 8, 128, 128], P('wide', 'narrow'), may hold values from -6 to 6
- previous: bfloat16 [8, 4, 3, 8, 128, 128], P('wide', 'narrow'), may hold values from -3 to 3
- slot_count: int32 [8, 4], P('wide', 'narrow'), may hold values from 1 to 3, as said below
- partner: int32 [8, 4, 3, 8], P('wide', 'narrow'), may hold values from -1 to 2, as said below
- face_size: int32 [8, 4, 3, 8], P('wide', 'narrow'), may hold values from 0 to 128, as said below
Outputs:
- solution: float32 [8, 4, 3, 8, 128, 128], P('wide', 'narrow')
- residual: float32 [8, 4, 3, 8, 128, 128], P('wide', 'narrow')
The draws below stay inside these ranges and needn't reach their ends.
Inputs may be any that keep to these rules, and one draw needn't show every extreme that they name: Slots of a device below its slot_count hold subdomains; the others are empty. partner names the slot of the subdomain across a face as in the reference program; the relation is symmetric (the partner face names this slot back), and it is -1 on empty slots, on faces whose partner slot is empty, on face 0 at narrow index 0 and on face 1 at the last narrow index. `face_size`: both sides of a face with a partner have the same size; faces of empty slots have size 0, all other faces at least 32.
All inputs are finite; a program needn't handle non-finite values.
Results may differ from the reference program's by a relative error of at most 0.00355.
The reference program's roundings to bfloat16 on the way count: a program that leaves them out, or rounds other values in their place, can miss the bound.
Values may be sent and summed in bfloat16 or wider, within the bound.
No kernel may reach another device: no remote copies, remote signals or barrier semaphores. Data moves between devices by JAX's collectives and lax.ppermute only.
A program may use at most 128 MiB of HBM per device.

```python
import math
import jax
import jax.numpy as jnp
from jax import lax

FW = 128
NF = 8
SLOTS = 3
NRHS = 128
NQ = 8
ITERS = 2
NB = 1024
SPACE = 8
SLABS = 4
NCG = 96
NT = 64


def look_up(table_in, slot_map):
    return jnp.take_along_axis(table_in, slot_map, axis=2)


def shift_below(table_in, filler):
    pad_row = jnp.full_like(table_in[:, :1], filler)
    return jnp.concatenate([pad_row, table_in[:, :-1]], axis=1)


def shift_above(table_in, filler):
    pad_row = jnp.full_like(table_in[:, :1], filler)
    return jnp.concatenate([table_in[:, 1:], pad_row], axis=1)


def layout_tables(seed_key):
    base_key = jax.random.fold_in(seed_key, 9173)
    levels = jax.random.randint(jax.random.fold_in(base_key, 1), (SPACE, SLABS), 0, 5)
    middle = max(1, SLOTS - 1)
    live_count = jnp.where(levels < 3, 1, jnp.where(levels == 3, middle, SLOTS)).astype(jnp.int32)
    slot_ids = jnp.arange(SLOTS, dtype=jnp.int32)
    alive_slot = slot_ids[None, None, :] < live_count[:, :, None]
    scores = jax.random.randint(jax.random.fold_in(base_key, 2), (SPACE, SLABS, 4, SLOTS), 0, 1 << 20) * SLOTS + slot_ids
    forward = jnp.argsort(scores, axis=-1).astype(jnp.int32)
    backward = jnp.argsort(forward, axis=-1).astype(jnp.int32)
    raw_sizes = jax.random.randint(jax.random.fold_in(base_key, 3), (SPACE, SLABS, SLOTS, NF), FW // 4, FW + 1).astype(jnp.int32)
    wide_next = forward[:, :, 0]
    wide_prev = jnp.roll(backward[:, :, 0], 1, axis=0)
    slab_next = forward[:, :, 1]
    slab_prev = shift_below(backward[:, :, 1], 0)
    slab_ids = jnp.arange(SLABS)
    has_above = (slab_ids < SLABS - 1)[None, :, None]
    has_below = (slab_ids > 0)[None, :, None]
    alive_right = jnp.roll(alive_slot, -1, axis=0)
    alive_left = jnp.roll(alive_slot, 1, axis=0)
    alive_above = shift_above(alive_slot, False)
    alive_below = shift_below(alive_slot, False)
    slot_maps = [slab_prev, slab_next, wide_prev, wide_next, forward[:, :, 2], backward[:, :, 2], forward[:, :, 3], backward[:, :, 3]]
    present = [has_below & look_up(alive_below, slab_prev), has_above & look_up(alive_above, slab_next), look_up(alive_left, wide_prev), look_up(alive_right, wide_next), look_up(alive_slot, forward[:, :, 2]), look_up(alive_slot, backward[:, :, 2]), look_up(alive_slot, forward[:, :, 3]), look_up(alive_slot, backward[:, :, 3])]
    present = [alive_slot & linked for linked in present]
    partner = jnp.stack([jnp.where(linked, slot_map, -1) for linked, slot_map in zip(present, slot_maps)], axis=-1).astype(jnp.int32)
    odd_sizes = [look_up(shift_below(raw_sizes[..., 1], 0), slab_prev), None, look_up(jnp.roll(raw_sizes[..., 3], 1, axis=0), wide_prev), None, look_up(raw_sizes[..., 5], forward[:, :, 2]), None, look_up(raw_sizes[..., 7], forward[:, :, 3]), None]
    size_list = []
    for face_id in range(8):
        own_size = raw_sizes[..., face_id]
        if face_id % 2 == 0:
            own_size = jnp.where(present[face_id], odd_sizes[face_id], own_size)
        size_list.append(own_size)
    face_size = jnp.where(alive_slot[..., None], jnp.stack(size_list, axis=-1), 0).astype(jnp.int32)
    return (live_count, partner, face_size)


def symmetric_blocks(seed_key, number_of, order, low, high, reach, target):

    def one_block(number):
        block_key = jax.random.fold_in(seed_key, number)
        noise = jax.random.normal(jax.random.fold_in(block_key, 1), (order, order), jnp.float32)
        coupling = (noise + noise.T) * (reach / (2.0 * math.sqrt(2.0 * order)))
        diagonal = jnp.exp(jax.random.uniform(jax.random.fold_in(block_key, 2), (order,), jnp.float32, math.log(low), math.log(high)))
        matrix = jnp.diag(diagonal) + coupling
        return matrix.astype(target)
    return lax.map(one_block, jnp.arange(number_of, dtype=jnp.int32))


def draw_slot_count(key, part):
    return layout_tables(key)[0]


def draw_partner(key, part):
    return layout_tables(key)[1]


def draw_face_size(key, part):
    return layout_tables(key)[2]


def draw_schur_matrix(key, part):
    blocks = symmetric_blocks(jax.random.fold_in(key, 11), SPACE * SLABS * SLOTS, NB, 1.5, 5.0, 1.2, jnp.bfloat16)
    return blocks.reshape(SPACE, SLABS, SLOTS, NB, NB)


def draw_face_inverse(key, part):
    blocks = symmetric_blocks(jax.random.fold_in(key, 23), SPACE * SLABS * SLOTS * NF, FW, 0.6, 1.5, 0.4, jnp.bfloat16)
    return blocks.reshape(SPACE, SLABS, SLOTS, NF, FW, FW)


def draw_coarse_group(key, part):
    return symmetric_blocks(jax.random.fold_in(key, 31), SPACE, NCG, 0.5, 2.0, 0.5, jnp.float32)


def draw_coarse_top(key, part):
    return symmetric_blocks(jax.random.fold_in(key, 37), 1, NT, 3.0, 6.0, 2.5, jnp.float32)[0]


def draw_deluxe(key, part):
    full_shape = (SPACE, SLABS, SLOTS, NF, FW, FW)
    noise = jax.random.normal(jax.random.fold_in(key, 41), full_shape, jnp.float32) * (0.35 / math.sqrt(FW))
    diagonal = jax.random.uniform(jax.random.fold_in(key, 43), full_shape[:-1], jnp.float32, 0.3, 0.8)
    identity = jnp.eye(FW, dtype=jnp.float32)
    return (noise + diagonal[..., None] * identity).astype(jnp.bfloat16)


def block_scale(stream_key, dims, shards, least, high):
    def one(position, parts):
        steps = jax.random.uniform(jax.random.fold_in(jax.random.fold_in(stream_key, 6), position), (parts,), jnp.float32, least / len(shards), high / len(shards))
        return jnp.repeat(jnp.exp(steps), dims[position] // parts).reshape((-1,) + (1,) * (len(dims) - position - 1))

    gain = one(*shards[0])
    for cut in shards[1:]:
        gain = gain * one(*cut)
    return gain


def scatter_about(own_key, shape, scale, bound, split=(), kind=jnp.bfloat16):
    drawn = scale * jax.random.normal(own_key, shape, jnp.float32)
    if split:
        drawn = drawn * block_scale(own_key, shape, split, -0.22, 0.18)
    return jnp.clip(drawn, -bound, bound).astype(kind)


def setup_inputs(seed: int = 0) -> dict:
    arg_keys = jax.random.split(jax.random.key(seed), 13)
    schur_matrix = draw_schur_matrix(jax.random.fold_in(arg_keys[12], 71), 0)
    face_inverse = draw_face_inverse(jax.random.fold_in(arg_keys[12], 71), 0)
    deluxe = draw_deluxe(jax.random.fold_in(arg_keys[12], 71), 0)
    primal_weight = jnp.clip(jnp.exp(math.log(0.3) - 1.7917595 * jax.random.uniform(arg_keys[3], (SPACE, SLABS, SLOTS, NF, FW), jnp.float32) ** block_scale(arg_keys[3], (SPACE, SLABS, SLOTS, NF, FW), ((0, 8), (1, 4)), -0.2, 0.2)), 0.05, 0.3)
    coarse_group = draw_coarse_group(jax.random.fold_in(arg_keys[12], 71), 0)
    coarse_map = scatter_about(arg_keys[5], (SPACE, NCG, NQ), NCG ** -0.5, 0.625, ((0, 8), (1, 4)), jnp.float32)
    coarse_top = draw_coarse_top(jax.random.fold_in(arg_keys[12], 71), 0)
    load_vector = scatter_about(arg_keys[7], (SPACE, SLABS, SLOTS, NF, FW, NRHS), 1.0, 6.0, ((0, 8), (1, 4)))
    previous = scatter_about(arg_keys[8], (SPACE, SLABS, SLOTS, NF, FW, NRHS), 0.5, 3.0, ((0, 8), (1, 4)))
    slot_count = draw_slot_count(jax.random.fold_in(arg_keys[12], 71), 0)
    partner = draw_partner(jax.random.fold_in(arg_keys[12], 71), 0)
    face_size = draw_face_size(jax.random.fold_in(arg_keys[12], 71), 0)
    return {"schur_matrix": schur_matrix, "face_inverse": face_inverse, "deluxe": deluxe, "primal_weight": primal_weight, "coarse_group": coarse_group, "coarse_map": coarse_map, "coarse_top": coarse_top, "load_vector": load_vector, "previous": previous, "slot_count": slot_count, "partner": partner, "face_size": face_size}


precise = lax.Precision.HIGHEST


def live_entries(slot_count, face_size):
    slot_ids = jnp.arange(SLOTS, dtype=jnp.int32)
    entry_ids = jnp.arange(FW, dtype=jnp.int32)
    slot_alive = slot_ids[None, None, :] < slot_count[:, :, None]
    inside = entry_ids[None, None, None, None, :] < face_size[:, :, :, :, None]
    both_live = jnp.logical_and(slot_alive[:, :, :, None, None], inside)
    return jnp.where(both_live, 1.0, 0.0).astype(jnp.float32)[..., None]


def partner_values(values, partner):
    zero_slab = jnp.zeros_like(values[:, :1, :, 0])
    from_below = jnp.concatenate([zero_slab, values[:, :-1, :, 1]], axis=1)
    from_above = jnp.concatenate([values[:, 1:, :, 0], zero_slab], axis=1)
    from_left = jnp.roll(values[:, :, :, 3], 1, axis=0)
    from_right = jnp.roll(values[:, :, :, 2], -1, axis=0)
    sources = jnp.stack([from_below, from_above, from_left, from_right, values[:, :, :, 5], values[:, :, :, 4], values[:, :, :, 7], values[:, :, :, 6]], axis=3)
    chosen = jnp.clip(partner, 0, SLOTS - 1).astype(jnp.int32)
    picked = jnp.take_along_axis(sources, chosen[:, :, :, :, None, None], axis=2)
    return jnp.where((partner >= 0)[:, :, :, :, None, None], picked, jnp.zeros_like(picked))


def apply_schur(schur_matrix, direction_half):
    blocks = schur_matrix.reshape(SPACE * SLABS * SLOTS, NB, NB)
    vectors = direction_half.reshape(SPACE * SLABS * SLOTS, NB, NRHS)

    def product(operands):
        return jnp.dot(operands[0], operands[1], preferred_element_type=jnp.float32)

    return lax.map(product, (blocks, vectors)).reshape(direction_half.shape)


def reference(schur_matrix, face_inverse, deluxe, primal_weight, coarse_group, coarse_map, coarse_top, load_vector, previous, slot_count, partner, face_size):
    live_mask = live_entries(slot_count, face_size)
    linked = (partner >= 0)[:, :, :, :, None, None]
    shared = jnp.where(linked, 0.5, 1.0).astype(jnp.float32)
    deluxe_full = deluxe.astype(jnp.float32)
    inverse_full = face_inverse.astype(jnp.float32)

    def assemble(values):
        return values + partner_values(values, partner)

    def global_inner(first_vec, second_vec):
        return jnp.sum(shared * first_vec * second_vec, axis=(0, 1, 2, 3, 4))

    def operator(values):
        return live_mask * apply_schur(schur_matrix, values.astype(jnp.bfloat16))

    def precondition(values):
        res_half = values.astype(jnp.bfloat16).astype(jnp.float32)
        scaled = live_mask * jnp.einsum("wnsfkj,wnsfkr->wnsfjr", deluxe_full, res_half)
        scaled_half = scaled.astype(jnp.bfloat16).astype(jnp.float32)
        local_part = jnp.einsum("wnsfjk,wnsfkr->wnsfjr", inverse_full, scaled_half)
        coarse_in = jnp.sum(primal_weight[..., None] * scaled, axis=4)
        group_vec = coarse_in.reshape(SPACE, NCG, NRHS)
        group_part = jnp.einsum("wcd,wdr->wcr", coarse_group, group_vec, precision=precise)
        restricted = jnp.einsum("wcq,wcr->wqr", coarse_map, group_vec, precision=precise).reshape(NT, NRHS)
        top_part = jnp.dot(coarse_top, restricted, precision=precise).reshape(SPACE, NQ, NRHS)
        coarse_out = group_part + jnp.einsum("wcq,wqr->wcr", coarse_map, top_part, precision=precise)
        coarse_out = coarse_out.reshape(SPACE, SLABS, SLOTS, NF, 1, NRHS)
        correction = local_part + primal_weight[..., None] * coarse_out
        corr_half = (live_mask * correction).astype(jnp.bfloat16).astype(jnp.float32)
        weighted = live_mask * jnp.einsum("wnsfjk,wnsfkr->wnsfjr", deluxe_full, corr_half)
        return assemble(weighted)

    prev_full = previous.astype(jnp.float32)
    prev_partner = partner_values(previous, partner).astype(jnp.float32)
    averaged = live_mask * jnp.where(linked, 0.5 * (prev_full + prev_partner), prev_full)
    residual = assemble(live_mask * load_vector.astype(jnp.float32) - operator(averaged))
    solution = averaged
    precond = precondition(residual)
    precond_norm = global_inner(residual, precond)
    direction = precond
    for iteration in range(ITERS):
        image_full = assemble(operator(direction))
        step_size = precond_norm / global_inner(direction, image_full)
        solution = solution + step_size * direction
        residual = residual - step_size * image_full
        if iteration + 1 < ITERS:
            precond = precondition(residual)
            next_norm = global_inner(residual, precond)
            direction = precond + (next_norm / precond_norm) * direction
            precond_norm = next_norm
    return solution, residual
```

```python
import jax
import jax.numpy as jnp
from jax import lax
from jax.experimental import pallas as pl
from jax.experimental.pallas import tpu as pltpu
from jax.sharding import PartitionSpec as P

precise = lax.Precision.HIGHEST
F32 = jnp.float32
BF16 = jnp.bfloat16
AXES = ("wide", "narrow")
VMEM = pl.BlockSpec(memory_space=pltpu.VMEM)
SMEM = pl.BlockSpec(memory_space=pltpu.SMEM)


def call(kernel, name, scalars, arrays, outs, scratch=()):
    return pl.pallas_call(
        kernel,
        name=name,
        in_specs=[SMEM] * len(scalars) + [VMEM] * len(arrays),
        out_specs=[VMEM] * len(outs),
        out_shape=[jax.ShapeDtypeStruct(shape, dtype) for shape, dtype in outs],
        scratch_shapes=list(scratch),
        compiler_params=pltpu.CompilerParams(vmem_limit_bytes=40 * 1024 * 1024),
    )(*scalars, *arrays)


def odd(axis):
    return lax.axis_index(axis) % 2 == 1


def from_face(own, got, slot, face):
    if face >= 4:
        return own[slot, face ^ 1]
    near, far = (got[0], got[1]) if face < 2 else (got[2], got[3])
    first = near[slot]
    second = far[slot]
    is_odd = odd("narrow") if face < 2 else odd("wide")
    if face % 2:
        return jnp.where(is_odd, second, first)
    return jnp.where(is_odd, first, second)


def send_faces(sends, slot, faces):
    odd_n = odd("narrow")
    odd_w = odd("wide")
    kind = sends[0].dtype
    sends[0][slot] = jnp.where(odd_n, faces[0], faces[1]).astype(kind)
    sends[1][slot] = jnp.where(odd_n, faces[1], faces[0]).astype(kind)
    sends[2][slot] = jnp.where(odd_w, faces[2], faces[3]).astype(kind)
    sends[3][slot] = jnp.where(odd_w, faces[3], faces[2]).astype(kind)


def live_rows(count, size, slot, face, shape):
    rows = lax.broadcasted_iota(jnp.int32, shape, 0)
    return rows < jnp.where(slot < count[0, 0], size[slot, face], 0)


def fold(values):
    rows, columns = values.shape
    return jnp.sum(values.reshape(rows // 8, 8, columns), axis=0)


def total_rows(gathered):
    return jnp.sum(gathered[...], axis=0)


def multiply(schur, vec, slot, width):
    span = 2 * width
    order = vec.shape[0]
    parts = []
    for start in range(0, order, span):
        block = jnp.dot(
            schur[slot, start : start + span], vec[...], preferred_element_type=F32
        )
        parts += [block[:width], block[width:]]
    return parts


def start_kernel(partner, size, count, previous, load, schur, g0, g1, g2, g3, averaged, local, s0, s1, s2, s3, vec):
    got = (g0, g1, g2, g3)
    slots, faces, width, columns = previous.shape

    def one_slot(slot, carry):
        for face in range(faces):
            other = partner[slot, face]
            mine = previous[slot, face].astype(F32)
            theirs = from_face(previous, got, jnp.maximum(other, 0), face).astype(F32)
            value = jnp.where(other >= 0, 0.5 * (mine + theirs), mine)
            value = jnp.where(live_rows(count, size, slot, face, mine.shape), value, 0.0)
            averaged[slot, face] = value
            vec[face * width : (face + 1) * width] = value.astype(BF16)
        products = multiply(schur, vec, slot, width)
        sent = []
        for face in range(faces):
            value = load[slot, face].astype(F32) - products[face]
            value = jnp.where(live_rows(count, size, slot, face, value.shape), value, 0.0)
            local[slot, face] = value
            if face < 4:
                sent.append(value)
        send_faces((s0, s1, s2, s3), slot, sent)
        return carry

    lax.fori_loop(0, slots, one_slot, 0)


def scale_slot(slot, values, partner_size, deluxe, spread_weight, scaled, coarse_in):
    count, size = partner_size
    rows = []
    for face, value in enumerate(values):
        part = lax.dot_general(
            deluxe[slot, face],
            value.astype(BF16),
            (((0,), (0,)), ((), ())),
            preferred_element_type=F32,
        )
        part = jnp.where(live_rows(count, size, slot, face, part.shape), part, 0.0)
        scaled[slot, face] = part.astype(BF16)
        rows.append(jnp.sum(spread_weight[slot, face] * part, axis=0, keepdims=True))
    faces = len(values)
    coarse_in[pl.ds(pl.multiple_of(slot * faces, 8), faces)] = jnp.concatenate(rows, axis=0)


def spread_restricted(coarse_map_t, coarse_in, restricted):
    part = jnp.dot(coarse_map_t[...], coarse_in[...], precision=precise, preferred_element_type=F32)
    restricted[...] = jnp.broadcast_to(part[None], restricted.shape)


def first_scale_kernel(partner, size, count, local, deluxe, spread_weight, coarse_map_t, g0, g1, g2, g3, residual, scaled, coarse_in, restricted):
    got = (g0, g1, g2, g3)
    slots, faces = local.shape[:2]

    def one_slot(slot, carry):
        values = []
        for face in range(faces):
            other = partner[slot, face]
            theirs = from_face(local, got, jnp.maximum(other, 0), face)
            value = local[slot, face] + jnp.where(other >= 0, theirs, 0.0)
            residual[slot, face] = value
            values.append(value)
        scale_slot(slot, values, (count, size), deluxe, spread_weight, scaled, coarse_in)
        return carry

    lax.fori_loop(0, slots, one_slot, 0)
    spread_restricted(coarse_map_t, coarse_in, restricted)


def next_scale_kernel(partner, size, count, old_residual, image, sums, deluxe, spread_weight, coarse_map_t, g0, g1, g2, g3, residual, full_image, scaled, coarse_in, restricted):
    got = (g0, g1, g2, g3)
    slots, faces = image.shape[:2]
    totals = total_rows(sums)
    step = totals[0:1] / totals[1:2]

    def one_slot(slot, carry):
        values = []
        for face in range(faces):
            other = partner[slot, face]
            theirs = from_face(image, got, jnp.maximum(other, 0), face).astype(F32)
            full = image[slot, face] + jnp.where(other >= 0, theirs, 0.0)
            full_image[slot, face] = full
            value = old_residual[slot, face] - step * full
            residual[slot, face] = value
            values.append(value)
        scale_slot(slot, values, (count, size), deluxe, spread_weight, scaled, coarse_in)
        return carry

    lax.fori_loop(0, slots, one_slot, 0)
    spread_restricted(coarse_map_t, coarse_in, restricted)


def inverse_kernel(scaled, face_inverse, local_part):
    slots, faces = scaled.shape[:2]

    def one_slot(slot, carry):
        for face in range(faces):
            local_part[slot, face] = jnp.dot(
                face_inverse[slot, face], scaled[slot, face], preferred_element_type=F32
            )
        return carry

    lax.fori_loop(0, slots, one_slot, 0)


def coarse_kernel_body(coarse_rows, restricted, coarse_group, coarse_map, coarse_top, group_vec):
    narrow = len(coarse_rows)
    each, columns = coarse_rows[0].shape
    here = lax.axis_index("narrow")
    for back, rows in enumerate(coarse_rows):
        place = (here + narrow - back) % narrow
        group_vec[pl.ds(pl.multiple_of(place * each, 8), each)] = rows[...]
    gathered = restricted[...]
    everyone = jnp.sum(
        gathered.reshape(gathered.shape[0] // narrow, narrow, gathered.shape[1], columns), axis=1
    ).reshape(-1, columns)
    top = jnp.dot(coarse_top[...], everyone, precision=precise, preferred_element_type=F32)
    group_part = jnp.dot(
        coarse_group[...], group_vec[...], precision=precise, preferred_element_type=F32
    )
    return group_part + jnp.dot(
        coarse_map[...], top, precision=precise, preferred_element_type=F32
    )


def make_weight_kernel(narrow):
    def weight_kernel(size, count, *refs):
        coarse_rows = refs[:narrow]
        restricted, coarse_group, coarse_map, coarse_top, local_part, spread_weight, deluxe = refs[
            narrow : narrow + 7
        ]
        weighted, s0, s1, s2, s3, group_vec, coarse_out = refs[narrow + 7 :]
        slots, faces = weighted.shape[:2]
        coarse_out[...] = coarse_kernel_body(
            coarse_rows, restricted, coarse_group, coarse_map, coarse_top, group_vec
        )

        def one_slot(slot, carry):
            sent = []
            for face in range(faces):
                row = coarse_out[pl.ds(slot * faces + face, 1)]
                value = local_part[slot, face] + spread_weight[slot, face] * row
                live = live_rows(count, size, slot, face, value.shape)
                value = jnp.where(live, value, 0.0).astype(BF16)
                value = jnp.dot(deluxe[slot, face], value, preferred_element_type=F32)
                value = jnp.where(live, value, 0.0)
                weighted[slot, face] = value
                if face < 4:
                    sent.append(value)
            send_faces((s0, s1, s2, s3), slot, sent)
            return carry

        lax.fori_loop(0, slots, one_slot, 0)

    return weight_kernel


def make_operator_kernel(later):
    def operator_kernel(partner, size, count, weighted, residual, schur, g0, g1, g2, g3, *refs):
        if later:
            old_direction, old_image = refs[:2]
            refs = refs[2:]
        direction, image, sums, s0, s1, s2, s3, vec = refs
        got = (g0, g1, g2, g3)
        slots, faces, width, columns = weighted.shape

        def one_slot(slot, carry):
            norm, curve, cross = carry
            for face in range(faces):
                other = partner[slot, face]
                mine = weighted[slot, face]
                theirs = from_face(weighted, got, jnp.maximum(other, 0), face)
                value = mine + jnp.where(other >= 0, theirs, 0.0)
                direction[slot, face] = value
                vec[face * width : (face + 1) * width] = value.astype(BF16)
                norm = norm + fold(residual[slot, face] * mine)
            products = multiply(schur, vec, slot, width)
            sent = []
            for face in range(faces):
                live = live_rows(count, size, slot, face, products[face].shape)
                value = jnp.where(live, products[face], 0.0)
                image[slot, face] = value
                curve = curve + fold(direction[slot, face] * value)
                if later:
                    cross = cross + fold(
                        direction[slot, face] * old_image[slot, face]
                        + old_direction[slot, face] * value
                    )
                if face < 4:
                    sent.append(value)
            send_faces((s0, s1, s2, s3), slot, sent)
            return norm, curve, cross

        zero = jnp.zeros((8, columns), F32)
        found = lax.fori_loop(0, slots, one_slot, (zero, zero, zero))
        rows = [jnp.sum(one, axis=0, keepdims=True) for one in found]
        rows.append(jnp.zeros((5, columns), F32))
        sums[...] = jnp.broadcast_to(jnp.concatenate(rows, axis=0)[None], sums.shape)

    return operator_kernel


def finish_kernel(partner, averaged, direction, precond, residual, full_image, image, first_sums, later_sums, g0, g1, g2, g3, solution_out, residual_out):
    got = (g0, g1, g2, g3)
    slots, faces = image.shape[:2]
    first = total_rows(first_sums)
    later = total_rows(later_sums)
    first_step = first[0:1] / first[1:2]
    ratio = later[0:1] / first[0:1]
    curve = later[1:2] + ratio * (later[2:3] + ratio * first[1:2])
    step = later[0:1] / curve
    old_step = first_step + step * ratio

    def one_slot(slot, carry):
        for face in range(faces):
            other = partner[slot, face]
            theirs = from_face(image, got, jnp.maximum(other, 0), face).astype(F32)
            full = image[slot, face] + jnp.where(other >= 0, theirs, 0.0)
            full = full + ratio * full_image[slot, face]
            residual_out[slot, face] = residual[slot, face] - step * full
            solution_out[slot, face] = (
                averaged[slot, face]
                + old_step * direction[slot, face]
                + step * precond[slot, face]
            )
        return carry

    lax.fori_loop(0, slots, one_slot, 0)


def body(
    schur_matrix,
    face_inverse,
    deluxe,
    primal_weight,
    coarse_group,
    coarse_map,
    coarse_top,
    load_vector,
    previous,
    slot_count,
    partner,
    face_size,
):
    schur_matrix = schur_matrix[0, 0]
    face_inverse = face_inverse[0, 0]
    deluxe = deluxe[0, 0]
    coarse_group = coarse_group[0]
    coarse_map = coarse_map[0]
    load_vector = load_vector[0, 0]
    previous = previous[0, 0]
    partner = partner[0, 0]
    face_size = face_size[0, 0]
    shape = load_vector.shape
    slots, faces, width, columns = shape
    order = schur_matrix.shape[1]
    quotient = coarse_map.shape[1]
    wide = lax.axis_size("wide")
    narrow = lax.axis_size("narrow")
    devices = wide * narrow
    one_face = (slots, width, columns)

    narrow_near = [(i, i ^ 1) for i in range(narrow)]
    narrow_far = [(i, i + 1 if i % 2 else i - 1) for i in range(1, narrow - 1)]
    wide_near = [(i, i ^ 1) for i in range(wide)]
    wide_far = [(i, (i + 1 if i % 2 else i - 1) % wide) for i in range(wide)]

    def swap(sends):
        return (
            lax.ppermute(sends[0], "narrow", narrow_near),
            lax.ppermute(sends[1], "narrow", narrow_far),
            lax.ppermute(sends[2], "wide", wide_near),
            lax.ppermute(sends[3], "wide", wide_far),
        )

    def from_all(spread):
        return lax.all_to_all(spread, AXES, 0, 0, tiled=False)

    def of_group(rows):
        got = [rows]
        for back in range(1, narrow):
            ring = [(i, (i + back) % narrow) for i in range(narrow)]
            got.append(lax.ppermute(rows, "narrow", ring))
        return got

    odd_n = odd("narrow")
    odd_w = odd("wide")
    got = swap(
        (
            jnp.where(odd_n, previous[:, 0], previous[:, 1]),
            jnp.where(odd_n, previous[:, 1], previous[:, 0]),
            jnp.where(odd_w, previous[:, 2], previous[:, 3]),
            jnp.where(odd_w, previous[:, 3], previous[:, 2]),
        )
    )
    spread_weight = jnp.broadcast_to(primal_weight[0, 0][..., None], shape)
    coarse_map_t = coarse_map.T
    ids = (partner, face_size, slot_count)
    vec = pltpu.VMEM((order, columns), BF16)
    sends_f32 = [(one_face, F32)] * 4
    averaged, local, *sends = call(
        start_kernel,
        "start",
        ids,
        (previous, load_vector, schur_matrix) + got,
        [(shape, F32), (shape, F32)] + sends_f32,
        [vec],
    )
    scale_outs = [
        (shape, BF16),
        ((slots * faces, columns), F32),
        ((devices, quotient, columns), F32),
    ]

    def weigh(scaled, coarse_in, restricted):
        restricted = from_all(restricted)
        coarse_rows = of_group(coarse_in)
        (local_part,) = call(
            inverse_kernel, "inverse", (), (scaled, face_inverse), [(shape, F32)]
        )
        weighted, *sends = call(
            make_weight_kernel(narrow),
            "weight",
            (face_size, slot_count),
            (
                *coarse_rows,
                restricted,
                coarse_group,
                coarse_map,
                coarse_top,
                local_part,
                spread_weight,
                deluxe,
            ),
            [(shape, F32)] + sends_f32,
            [
                pltpu.VMEM((narrow * slots * faces, columns), F32),
                pltpu.VMEM((slots * faces, columns), F32),
            ],
        )
        return weighted, swap(sends)

    sum_out = ((devices, 8, columns), F32)
    residual, scaled, coarse_in, restricted = call(
        first_scale_kernel,
        "first_scale",
        ids,
        (local, deluxe, spread_weight, coarse_map_t) + swap(sends),
        [(shape, F32)] + scale_outs,
    )
    weighted, got = weigh(scaled, coarse_in, restricted)
    direction, image, first_sums, *sends = call(
        make_operator_kernel(False),
        "first_operator",
        ids,
        (weighted, residual, schur_matrix) + got,
        [(shape, F32), (shape, F32), sum_out] + sends_f32,
        [vec],
    )
    first_sums = from_all(first_sums)
    residual, full_image, scaled, coarse_in, restricted = call(
        next_scale_kernel,
        "next_scale",
        ids,
        (residual, image, first_sums, deluxe, spread_weight, coarse_map_t) + swap(sends),
        [(shape, F32), (shape, F32)] + scale_outs,
    )
    weighted, got = weigh(scaled, coarse_in, restricted)
    precond, later_image, later_sums, *sends = call(
        make_operator_kernel(True),
        "later_operator",
        ids,
        (weighted, residual, schur_matrix) + got + (direction, image),
        [(shape, F32), (shape, F32), sum_out] + [(one_face, BF16)] * 4,
        [vec],
    )
    later_sums = from_all(later_sums)
    solution, residual = call(
        finish_kernel,
        "finish",
        (partner,),
        (averaged, direction, precond, residual, full_image, later_image, first_sums, later_sums)
        + swap(sends),
        [(shape, F32), (shape, F32)],
    )
    return (solution[None, None], residual[None, None])


def solution(mesh):
    in_specs = (
        P("wide", "narrow", None, None, None),
        P("wide", "narrow", None, None, None, None),
        P("wide", "narrow", None, None, None, None),
        P("wide", "narrow", None, None, None),
        P("wide", "narrow", None),
        P("wide", "narrow", None),
        P("wide", None),
        P("wide", "narrow", None, None, None, None),
        P("wide", "narrow", None, None, None, None),
        P("wide", "narrow"),
        P("wide", "narrow", None, None),
        P("wide", "narrow", None, None),
    )
    out_specs = (
        P("wide", "narrow", None, None, None, None),
        P("wide", "narrow", None, None, None, None),
    )
    return jax.shard_map(body, mesh=mesh, in_specs=in_specs, out_specs=out_specs, check_vma=False)
```

```python
import functools

import jax
import jax.numpy as jnp
from jax import lax
from jax.experimental import pallas as pl
from jax.experimental.pallas import tpu as pltpu
from jax.sharding import PartitionSpec as P

precise = lax.Precision.HIGHEST
F32 = jnp.float32
BF16 = jnp.bfloat16
VMEM = pl.BlockSpec(memory_space=pltpu.VMEM)
SMEM = pl.BlockSpec(memory_space=pltpu.SMEM)


def call(kernel, scalars, arrays, outs, scratch=()):
    return pl.pallas_call(
        kernel,
        in_specs=[SMEM] * len(scalars) + [VMEM] * len(arrays),
        out_specs=[VMEM] * len(outs),
        out_shape=[jax.ShapeDtypeStruct(shape, dtype) for shape, dtype in outs],
        scratch_shapes=list(scratch),
        compiler_params=pltpu.CompilerParams(vmem_limit_bytes=16 * 1024 * 1024),
    )(*scalars, *arrays)


def odd(axis):
    return lax.axis_index(axis) % 2 == 1


def from_face(own, got, slot, face):
    if face >= 4:
        return own[slot, face ^ 1]
    return from_device(got, face, slot * own.shape[2], own.shape[2])


def from_device(got, face, start, count):
    near, far = (got[0], got[1]) if face < 2 else (got[2], got[3])
    rows = pl.ds(pl.multiple_of(start, 8), count)
    is_odd = odd("narrow") if face < 2 else odd("wide")
    if face % 2:
        return jnp.where(is_odd, far[rows], near[rows])
    return jnp.where(is_odd, near[rows], far[rows])


def send_faces(sends, slot, faces):
    odd_n = odd("narrow")
    odd_w = odd("wide")
    kind = sends[0].dtype
    width = faces[0].shape[0]
    rows = pl.ds(pl.multiple_of(slot * width, width), width)
    sends[0][rows] = jnp.where(odd_n, faces[0], faces[1]).astype(kind)
    sends[1][rows] = jnp.where(odd_n, faces[1], faces[0]).astype(kind)
    sends[2][rows] = jnp.where(odd_w, faces[2], faces[3]).astype(kind)
    sends[3][rows] = jnp.where(odd_w, faces[3], faces[2]).astype(kind)


def chunks(total, columns):
    return [(start, min(columns, total - start)) for start in range(0, total, columns)]


class Pack:
    def __init__(self, start, columns, weight, group, map_t, top):
        self.columns = columns
        self.sizes = [weight, group, map_t, top]
        self.starts = []
        for rows, lanes in self.sizes:
            self.starts.append(start)
            start += rows * len(chunks(lanes, columns))
        self.end = start

    def store(self, sends, refs):
        for start, (rows, lanes), ref in zip(self.starts, self.sizes, refs):
            for number, (lane, many) in enumerate(chunks(lanes, self.columns)):
                value = ref[:, lane : lane + many]
                if many < self.columns:
                    filler = jnp.zeros((rows, self.columns - many), F32)
                    value = jnp.concatenate([value, filler], axis=1)
                for send in sends:
                    send[start + number * rows : start + (number + 1) * rows] = value

    def read(self, got, face, part):
        rows, lanes = self.sizes[part]
        pieces = []
        for number, (lane, many) in enumerate(chunks(lanes, self.columns)):
            value = from_device(got, face, self.starts[part] + number * rows, rows)
            pieces.append(value[:, :many])
        return pieces[0] if len(pieces) == 1 else jnp.concatenate(pieces, axis=1)


def exact(first, second):
    return jnp.dot(first, second, precision=precise, preferred_element_type=F32)


def exact_t(first, second):
    return lax.dot_general(
        first,
        second,
        (((0,), (0,)), ((), ())),
        precision=precise,
        preferred_element_type=F32,
    )


def send_kernel(previous, deluxe, face_inverse, s0, s1, s2, s3, sems):
    odd_n = lax.axis_index("narrow") % 2
    odd_w = lax.axis_index("wide") % 2
    slots, _, width, _ = previous.shape
    copies = []
    for send, face in ((s0, 1 - odd_n), (s1, odd_n), (s2, 3 - odd_w), (s3, 2 + odd_w)):
        for part, source in enumerate((previous, deluxe, face_inverse)):
            for slot in range(slots):
                row = (part * slots + slot) * width
                copies.append(
                    pltpu.make_async_copy(
                        source.at[slot, face],
                        send.at[pl.ds(row, width)],
                        sems.at[len(copies)],
                    )
                )
    for copy in copies:
        copy.start()
    for copy in copies:
        copy.wait()


def live_rows(count, size, slot, face, shape):
    rows = lax.broadcasted_iota(jnp.int32, shape, 0)
    return rows < jnp.where(slot < count[0, 0], size[slot, face], 0)


def fold(values):
    rows, columns = values.shape
    return jnp.sum(values.reshape(rows // 8, 8, columns), axis=0)


def multiply(schur, vec, slot, width):
    span = 2 * width
    order = vec.shape[0]
    parts = []
    for start in range(0, order, span):
        block = jnp.dot(
            schur[slot, start : start + span], vec[...], preferred_element_type=F32
        )
        parts += [block[:width], block[width:]]
    return parts


def start_kernel(pack, partner, size, count, previous, load, schur, weight, group, map_t, top, g0, g1, g2, g3, averaged, local, s0, s1, s2, s3, vec):
    got = (g0, g1, g2, g3)
    pack.store((s0, s1, s2, s3), (weight, group, map_t, top))
    slots, faces, width, _ = previous.shape

    def one_slot(slot, carry):
        for face in range(faces):
            other = partner[slot, face]
            mine = previous[slot, face].astype(F32)
            theirs = from_face(previous, got, jnp.maximum(other, 0), face).astype(F32)
            value = jnp.where(other >= 0, 0.5 * (mine + theirs), mine)
            value = jnp.where(live_rows(count, size, slot, face, mine.shape), value, 0.0)
            averaged[slot, face] = value
            vec[face * width : (face + 1) * width] = value.astype(BF16)
        products = multiply(schur, vec, slot, width)
        sent = []
        for face in range(faces):
            value = load[slot, face].astype(F32) - products[face]
            value = jnp.where(live_rows(count, size, slot, face, value.shape), value, 0.0)
            local[slot, face] = value
            if face < 4:
                sent.append(value)
        send_faces((s0, s1, s2, s3), slot, sent)
        return carry

    lax.fori_loop(0, slots, one_slot, 0)


def scale_slot(slot, values, ids, deluxe, spread_weight, given, scaled, coarse_in):
    partner, count, size = ids
    rows = []
    faces = len(values)
    slots, _, width, _ = deluxe.shape
    for face, value in enumerate(values):
        half = value.astype(BF16)
        blocks = [deluxe[slot, face]]
        if face < 4:
            other = jnp.maximum(partner[slot, face], 0)
            blocks.append(from_device(given, face, (slots + other) * width, width))
        for side, block in enumerate(blocks):
            part = lax.dot_general(
                block, half, (((0,), (0,)), ((), ())), preferred_element_type=F32
            )
            part = jnp.where(live_rows(count, size, slot, face, part.shape), part, 0.0)
            scaled[slot, face + side * faces] = part.astype(BF16)
            if side == 0:
                rows.append(jnp.sum(spread_weight[slot, face] * part, axis=0, keepdims=True))
    coarse_in[pl.ds(pl.multiple_of(slot * faces, 8), faces)] = jnp.concatenate(rows, axis=0)


def restrict(coarse_map_t, coarse_in):
    count = coarse_map_t.shape[1]
    coarse_in[count:] = jnp.dot(
        coarse_map_t[...], coarse_in[:count], precision=precise, preferred_element_type=F32
    )


def first_scale_kernel(partner, size, count, local, deluxe, spread_weight, coarse_map_t, *refs):
    got, given = refs[:4], refs[4:8]
    residual, scaled, coarse_in = refs[8:]
    slots, faces = local.shape[:2]

    def one_slot(slot, carry):
        values = []
        for face in range(faces):
            other = partner[slot, face]
            theirs = from_face(local, got, jnp.maximum(other, 0), face)
            value = local[slot, face] + jnp.where(other >= 0, theirs, 0.0)
            residual[slot, face] = value
            values.append(value)
        scale_slot(slot, values, (partner, count, size), deluxe, spread_weight, given, scaled, coarse_in)
        return carry

    lax.fori_loop(0, slots, one_slot, 0)
    restrict(coarse_map_t, coarse_in)


def next_scale_kernel(partner, size, count, old_residual, image, sums, deluxe, spread_weight, coarse_map_t, *refs):
    got, given = refs[:4], refs[4:8]
    residual, full_image, scaled, coarse_in = refs[8:]
    slots, faces = image.shape[:2]
    totals = sums[...]
    step = totals[0:1] / totals[1:2]

    def one_slot(slot, carry):
        values = []
        for face in range(faces):
            other = partner[slot, face]
            theirs = from_face(image, got, jnp.maximum(other, 0), face).astype(F32)
            full = image[slot, face] + jnp.where(other >= 0, theirs, 0.0)
            full_image[slot, face] = full
            value = old_residual[slot, face] - step * full
            residual[slot, face] = value
            values.append(value)
        scale_slot(slot, values, (partner, count, size), deluxe, spread_weight, given, scaled, coarse_in)
        return carry

    lax.fori_loop(0, slots, one_slot, 0)
    restrict(coarse_map_t, coarse_in)


def inverse_kernel(partner, scaled, face_inverse, g0, g1, g2, g3, local_part):
    given = (g0, g1, g2, g3)
    slots, faces, width, _ = face_inverse.shape

    def one_slot(slot, carry):
        for face in range(faces + 4):
            if face < faces:
                block = face_inverse[slot, face]
            else:
                other = jnp.maximum(partner[slot, face - faces], 0)
                block = from_device(given, face - faces, (2 * slots + other) * width, width)
            local_part[slot, face] = jnp.dot(
                block, scaled[slot, face], preferred_element_type=F32
            )
        return carry

    lax.fori_loop(0, slots, one_slot, 0)


def across_weight_kernel(pack, partner, g0, g1, g2, g3, spread):
    got = (g0, g1, g2, g3)
    slots, faces, width, columns = spread.shape
    for face in range(faces):
        rows = pack.read(got, face, 0)
        for slot in range(slots):
            other = partner[slot, face]
            row = jnp.zeros((1, width), F32)
            for place in range(slots):
                number = place * (pack.sizes[0][0] // slots) + (face ^ 1)
                row = jnp.where(other == place, rows[number : number + 1], row)
            spread[slot, face] = jnp.broadcast_to(row, (columns, width)).T


def make_group_kernel(pack, narrow, slots):
    def group_kernel(*refs):
        rows_of = refs[:narrow]
        coarse_group = refs[narrow]
        got = refs[narrow + 1 : narrow + 5]
        packed, group_part, group_vec = refs[narrow + 5 :]
        each = coarse_group.shape[0]
        faces = each // slots
        here = lax.axis_index("narrow")
        restricted = None
        for back, rows in enumerate(rows_of):
            place = (here + narrow - back) % narrow
            group_vec[pl.ds(pl.multiple_of(place * each, 8), each)] = rows[:each]
            part = rows[each:]
            restricted = part if restricted is None else restricted + part
        group = jnp.concatenate(
            [coarse_group[...], pack.read(got, 0, 1), pack.read(got, 1, 1)], axis=0
        )
        part = exact(group, group_vec[...])
        group_part[...] = part
        picked = [
            part[slot * faces + face : slot * faces + face + 1]
            for face in (2, 3)
            for slot in range(slots)
        ]
        quotient, columns = restricted.shape
        filler = packed.shape[0] - quotient - len(picked)
        packed[...] = jnp.concatenate(
            [restricted] + picked + [jnp.zeros((filler, columns), F32)], axis=0
        )

    return group_kernel


def make_apply_kernel(pack, halves, later):
    def apply_kernel(partner, size, count, *refs):
        pairs = refs[:halves]
        refs = refs[halves:]
        group_part, map_t, coarse_top, local_part, spread_weight, across_weight, deluxe = refs[:7]
        given, packs = refs[7:11], refs[11:15]
        residual, schur = refs[15:17]
        refs = refs[17:]
        if later:
            old_direction, old_image = refs[:2]
            refs = refs[2:]
        direction, image, sums, s0, s1, s2, s3 = refs[:7]
        weighted, everyone, every_pack, coarse_out, vec = refs[7:]
        slots, faces, width, columns = direction.shape
        quotient, each = map_t.shape
        here = lax.axis_index("wide")
        wide = 2 * halves
        packed = pairs[0].shape[0] // 2
        for half, rows in enumerate(pairs):
            for other in range(2):
                place = here ^ (2 * half + other)
                block = rows[other * packed : (other + 1) * packed]
                everyone[pl.ds(pl.multiple_of(place * quotient, 8), quotient)] = block[:quotient]
                every_pack[pl.ds(pl.multiple_of(place * packed, 8), packed)] = block
        tops = exact(
            jnp.concatenate(
                [coarse_top[...], pack.read(packs, 2, 3), pack.read(packs, 3, 3)], axis=0
            ),
            everyone[...],
        )
        own_top = tops[:quotient]
        coarse_out[:each] = group_part[:each] + exact_t(map_t[...], own_top)
        for face in range(4):
            top = own_top if face < 2 else tops[(face - 1) * quotient : face * quotient]
            value = exact_t(pack.read(packs, face, 2), top)
            start = (face + 1) * each
            if face < 2:
                value = value + group_part[start : start + each]
            coarse_out[start : start + each] = value

        def coarse_row(face, other):
            row = coarse_out[pl.ds((face + 1) * each + other * faces + (face ^ 1), 1)]
            if face < 2:
                return row
            side = here + wide - 1 if face == 2 else here + 1
            start = (side % wide) * packed + quotient + (slots if face == 2 else 0)
            return row + every_pack[pl.ds(start + other, 1)]

        def weigh(part, weight, row, block, live):
            value = part + weight * row
            value = jnp.where(live, value, 0.0).astype(BF16)
            value = jnp.dot(block, value, preferred_element_type=F32)
            return jnp.where(live, value, 0.0)

        def weigh_slot(slot, carry):
            for face in range(faces):
                live = live_rows(count, size, slot, face, (width, columns))
                weighted[slot, face] = weigh(
                    local_part[slot, face],
                    spread_weight[slot, face],
                    coarse_out[pl.ds(slot * faces + face, 1)],
                    deluxe[slot, face],
                    live,
                )
                if face < 4:
                    other = partner[slot, face]
                    place = jnp.maximum(other, 0)
                    theirs = weigh(
                        local_part[slot, faces + face],
                        across_weight[slot, face],
                        coarse_row(face, place),
                        from_device(given, face, (slots + place) * width, width),
                        live,
                    )
                    direction[slot, face] = jnp.where(other >= 0, theirs, 0.0)
            return carry

        lax.fori_loop(0, slots, weigh_slot, 0)

        def one_slot(slot, carry):
            norm, curve, cross = carry
            for face in range(faces):
                other = partner[slot, face]
                mine = weighted[slot, face]
                if face < 4:
                    value = mine + direction[slot, face]
                else:
                    theirs = weighted[jnp.maximum(other, 0), face ^ 1]
                    value = mine + jnp.where(other >= 0, theirs, 0.0)
                direction[slot, face] = value
                vec[face * width : (face + 1) * width] = value.astype(BF16)
                norm = norm + fold(residual[slot, face] * mine)
            products = multiply(schur, vec, slot, width)
            sent = []
            for face in range(faces):
                live = live_rows(count, size, slot, face, products[face].shape)
                value = jnp.where(live, products[face], 0.0)
                image[slot, face] = value
                curve = curve + fold(direction[slot, face] * value)
                if later:
                    cross = cross + fold(
                        direction[slot, face] * old_image[slot, face]
                        + old_direction[slot, face] * value
                    )
                if face < 4:
                    sent.append(value)
            send_faces((s0, s1, s2, s3), slot, sent)
            return norm, curve, cross

        zero = jnp.zeros((8, columns), F32)
        found = lax.fori_loop(0, slots, one_slot, (zero, zero, zero))
        rows = [jnp.sum(one, axis=0, keepdims=True) for one in found]
        rows.append(jnp.zeros((5, columns), F32))
        sums[...] = jnp.concatenate(rows, axis=0)

    return apply_kernel


def finish_kernel(partner, averaged, direction, precond, residual, full_image, image, first_sums, later_sums, g0, g1, g2, g3, solution_out, residual_out):
    got = (g0, g1, g2, g3)
    slots, faces = image.shape[:2]
    first = first_sums[...]
    later = later_sums[...]
    first_step = first[0:1] / first[1:2]
    ratio = later[0:1] / first[0:1]
    curve = later[1:2] + ratio * (later[2:3] + ratio * first[1:2])
    step = later[0:1] / curve
    old_step = first_step + step * ratio

    def one_slot(slot, carry):
        for face in range(faces):
            other = partner[slot, face]
            theirs = from_face(image, got, jnp.maximum(other, 0), face).astype(F32)
            full = image[slot, face] + jnp.where(other >= 0, theirs, 0.0)
            full = full + ratio * full_image[slot, face]
            residual_out[slot, face] = residual[slot, face] - step * full
            solution_out[slot, face] = (
                averaged[slot, face]
                + old_step * direction[slot, face]
                + step * precond[slot, face]
            )
        return carry

    lax.fori_loop(0, slots, one_slot, 0)


def body(
    schur_matrix,
    face_inverse,
    deluxe,
    primal_weight,
    coarse_group,
    coarse_map,
    coarse_top,
    load_vector,
    previous,
    slot_count,
    partner,
    face_size,
):
    schur_matrix = schur_matrix[0, 0]
    face_inverse = face_inverse[0, 0]
    deluxe = deluxe[0, 0]
    coarse_group = coarse_group[0]
    coarse_map = coarse_map[0]
    load_vector = load_vector[0, 0]
    previous = previous[0, 0]
    partner = partner[0, 0]
    face_size = face_size[0, 0]
    shape = load_vector.shape
    slots, faces, width, columns = shape
    order = schur_matrix.shape[1]
    quotient = coarse_map.shape[1]
    wide = lax.axis_size("wide")
    narrow = lax.axis_size("narrow")
    one_face = (slots * width, columns)
    each = slots * faces
    pack = Pack(
        slots * width,
        columns,
        (each, width),
        coarse_group.shape,
        (quotient, each),
        coarse_top.shape,
    )

    narrow_near = [(i, i ^ 1) for i in range(narrow)]
    narrow_far = [(i, i + 1 if i % 2 else i - 1) for i in range(1, narrow - 1)]
    wide_near = [(i, i ^ 1) for i in range(wide)]
    wide_far = [(i, (i + 1 if i % 2 else i - 1) % wide) for i in range(wide)]

    def swap(sends):
        return (
            lax.ppermute(sends[0], "narrow", narrow_near),
            lax.ppermute(sends[1], "narrow", narrow_far),
            lax.ppermute(sends[2], "wide", wide_near),
            lax.ppermute(sends[3], "wide", wide_far),
        )

    def of_group(rows):
        got = [rows]
        for back in range(1, narrow):
            ring = [(i, (i + back) % narrow) for i in range(narrow)]
            got.append(lax.ppermute(rows, "narrow", ring))
        return got

    def across(rows, step):
        return lax.ppermute(rows, "wide", [(i, i ^ step) for i in range(wide)])

    def total_and_swap(rows, sends):
        rows = sum(of_group(rows))
        got = swap(sends)
        rows = rows + across(rows, 1)
        rows = sum([rows] + [across(rows, step) for step in range(2, wide, 2)])
        return rows, got

    given = swap(
        pl.pallas_call(
            send_kernel,
            name="send",
            in_specs=[pl.BlockSpec(memory_space=pl.ANY)] * 3,
            out_specs=[VMEM] * 4,
            out_shape=[jax.ShapeDtypeStruct((3 * slots * width, columns), BF16)] * 4,
            scratch_shapes=[pltpu.SemaphoreType.DMA((12 * slots,))],
        )(previous, deluxe, face_inverse)
    )
    flat_weight = primal_weight[0, 0].reshape(each, width)
    spread_weight = jnp.broadcast_to(primal_weight[0, 0][..., None], shape)
    coarse_map_t = coarse_map.T
    ids = (partner, face_size, slot_count)
    vec = pltpu.VMEM((order, columns), BF16)
    averaged, local, *sends = call(
        functools.partial(start_kernel, pack),
        ids,
        (previous, load_vector, schur_matrix, flat_weight, coarse_group, coarse_map_t, coarse_top)
        + given,
        [(shape, F32), (shape, F32)] + [((pack.end, columns), F32)] * 4,
        [vec],
    )
    wider = (slots, faces + 4, width, columns)
    scale_outs = [(wider, BF16), ((each + quotient, columns), F32)]
    packed_rows = -(-(quotient + 2 * slots) // 8) * 8
    packs = swap(sends)
    (across_weight,) = call(
        functools.partial(across_weight_kernel, pack),
        (partner,),
        packs,
        [((slots, 4, width, columns), F32)],
    )

    def apply_to(later, scaled, coarse_in, more, send_type):
        rows_of = of_group(coarse_in)
        (local_part,) = call(
            inverse_kernel, (partner,), (scaled, face_inverse) + given, [(wider, F32)]
        )
        packed, group_part = call(
            make_group_kernel(pack, narrow, slots),
            (),
            (*rows_of, coarse_group) + packs,
            [((packed_rows, columns), F32), ((3 * each, columns), F32)],
            [pltpu.VMEM((narrow * each, columns), F32)],
        )
        pair = jnp.concatenate([packed, across(packed, 1)], axis=0)
        pairs = [pair] + [across(pair, step) for step in range(2, wide, 2)]
        return call(
            make_apply_kernel(pack, wide // 2, later),
            ids,
            (
                *pairs,
                group_part,
                coarse_map_t,
                coarse_top,
                local_part,
                spread_weight,
                across_weight,
                deluxe,
            )
            + given
            + packs
            + more,
            [(shape, F32), (shape, F32), ((8, columns), F32)] + [(one_face, send_type)] * 4,
            [
                pltpu.VMEM(shape, F32),
                pltpu.VMEM((wide * quotient, columns), F32),
                pltpu.VMEM((wide * packed_rows, columns), F32),
                pltpu.VMEM((5 * each, columns), F32),
                vec,
            ],
        )

    residual, scaled, coarse_in = call(
        first_scale_kernel,
        ids,
        (local, deluxe, spread_weight, coarse_map_t) + packs + given,
        [(shape, F32)] + scale_outs,
    )
    direction, image, first_sums, *sends = apply_to(
        False, scaled, coarse_in, (residual, schur_matrix), F32
    )
    first_sums, got = total_and_swap(first_sums, sends)
    residual, full_image, scaled, coarse_in = call(
        next_scale_kernel,
        ids,
        (residual, image, first_sums, deluxe, spread_weight, coarse_map_t) + got + given,
        [(shape, F32), (shape, F32)] + scale_outs,
    )
    precond, later_image, later_sums, *sends = apply_to(
        True, scaled, coarse_in, (residual, schur_matrix, direction, image), BF16
    )
    later_sums, got = total_and_swap(later_sums, sends)
    solution, residual = call(
        finish_kernel,
        (partner,),
        (averaged, direction, precond, residual, full_image, later_image, first_sums, later_sums)
        + got,
        [(shape, F32), (shape, F32)],
    )
    return (solution[None, None], residual[None, None])


def solution(mesh):
    in_specs = (
        P("wide", "narrow", None, None, None),
        P("wide", "narrow", None, None, None, None),
        P("wide", "narrow", None, None, None, None),
        P("wide", "narrow", None, None, None),
        P("wide", "narrow", None),
        P("wide", "narrow", None),
        P("wide", None),
        P("wide", "narrow", None, None, None, None),
        P("wide", "narrow", None, None, None, None),
        P("wide", "narrow"),
        P("wide", "narrow", None, None),
        P("wide", "narrow", None, None),
    )
    out_specs = (
        P("wide", "narrow", None, None, None, None),
        P("wide", "narrow", None, None, None, None),
    )
    return jax.shard_map(body, mesh=mesh, in_specs=in_specs, out_specs=out_specs, check_vma=False)
```

```python
import functools

import jax
import jax.numpy as jnp
from jax import lax
from jax.experimental import pallas as pl
from jax.experimental.pallas import tpu as pltpu
from jax.sharding import PartitionSpec as P

precise = lax.Precision.HIGHEST
COST = pl.CostEstimate(flops=1 << 30, bytes_accessed=0, transcendentals=0)
F32 = jnp.float32
BF16 = jnp.bfloat16
VMEM = pl.BlockSpec(memory_space=pltpu.VMEM)
SMEM = pl.BlockSpec(memory_space=pltpu.SMEM)


def call(kernel, scalars, arrays, outs, scratch=()):
    return pl.pallas_call(
        kernel,
        in_specs=[SMEM] * len(scalars) + [VMEM] * len(arrays),
        out_specs=[VMEM] * len(outs),
        out_shape=[jax.ShapeDtypeStruct(shape, dtype) for shape, dtype in outs],
        scratch_shapes=list(scratch),
        compiler_params=pltpu.CompilerParams(vmem_limit_bytes=16 * 1024 * 1024),
        cost_estimate=COST,
    )(*scalars, *arrays)


def odd(axis):
    return lax.axis_index(axis) % 2 == 1


def from_face(own, got, slot, face):
    if face >= 4:
        return own[slot, face ^ 1]
    return from_device(got, face, slot * own.shape[2], own.shape[2])


def from_device(got, face, start, count):
    near, far = (got[0], got[1]) if face < 2 else (got[2], got[3])
    rows = pl.ds(pl.multiple_of(start, 8), count)
    is_odd = odd("narrow") if face < 2 else odd("wide")
    if face % 2:
        return jnp.where(is_odd, far[rows], near[rows])
    return jnp.where(is_odd, near[rows], far[rows])


def send_faces(sends, slot, faces):
    odd_n = odd("narrow")
    odd_w = odd("wide")
    kind = sends[0].dtype
    width = faces[0].shape[0]
    rows = pl.ds(pl.multiple_of(slot * width, width), width)
    sends[0][rows] = jnp.where(odd_n, faces[0], faces[1]).astype(kind)
    sends[1][rows] = jnp.where(odd_n, faces[1], faces[0]).astype(kind)
    sends[2][rows] = jnp.where(odd_w, faces[2], faces[3]).astype(kind)
    sends[3][rows] = jnp.where(odd_w, faces[3], faces[2]).astype(kind)


def chunks(total, columns):
    return [(start, min(columns, total - start)) for start in range(0, total, columns)]


class Pack:
    def __init__(self, start, columns, weight, group, map_t, top):
        self.columns = columns
        self.sizes = [weight, group, map_t, top]
        self.starts = []
        for rows, lanes in self.sizes:
            self.starts.append(start)
            start += rows * len(chunks(lanes, columns))
        self.end = start

    def store(self, sends, refs):
        for start, (rows, lanes), ref in zip(self.starts, self.sizes, refs):
            for number, (lane, many) in enumerate(chunks(lanes, self.columns)):
                value = ref[:, lane : lane + many]
                if many < self.columns:
                    filler = jnp.zeros((rows, self.columns - many), F32)
                    value = jnp.concatenate([value, filler], axis=1)
                for send in sends:
                    send[start + number * rows : start + (number + 1) * rows] = value

    def read(self, got, face, part):
        rows, lanes = self.sizes[part]
        pieces = []
        for number, (lane, many) in enumerate(chunks(lanes, self.columns)):
            value = from_device(got, face, self.starts[part] + number * rows, rows)
            pieces.append(value[:, :many])
        return pieces[0] if len(pieces) == 1 else jnp.concatenate(pieces, axis=1)


def exact(first, second):
    return jnp.dot(first, second, precision=precise, preferred_element_type=F32)


def exact_t(first, second):
    return lax.dot_general(
        first,
        second,
        (((0,), (0,)), ((), ())),
        precision=precise,
        preferred_element_type=F32,
    )


def send_kernel(*refs):
    sources, sends = refs[:-4], refs[-4:]
    slots = sources[0].shape[0]
    for part, source in enumerate(sources):
        for slot in range(slots):
            send_faces(sends, part * slots + slot, [source[slot, face] for face in range(4)])


def live_rows(count, size, slot, face, shape):
    rows = lax.broadcasted_iota(jnp.int32, shape, 0)
    return rows < jnp.where(slot < count[0, 0], size[slot, face], 0)


def fold(values):
    rows, columns = values.shape
    return jnp.sum(values.reshape(rows // 8, 8, columns), axis=0)


def multiply(schur, vec, slot, width):
    span = 2 * width
    order = vec.shape[0]
    parts = []
    for start in range(0, order, span):
        block = jnp.dot(
            schur[slot, start : start + span], vec[...], preferred_element_type=F32
        )
        parts += [block[:width], block[width:]]
    return parts


def start_kernel(pack, partner, size, count, previous, load, schur, weight, group, map_t, top, g0, g1, g2, g3, averaged, local, s0, s1, s2, s3, vec):
    got = (g0, g1, g2, g3)
    pack.store((s0, s1, s2, s3), (weight, group, map_t, top))
    slots, faces, width, _ = previous.shape

    for slot in range(slots):
        for face in range(faces):
            other = partner[slot, face]
            mine = previous[slot, face].astype(F32)
            theirs = from_face(previous, got, jnp.maximum(other, 0), face).astype(F32)
            value = jnp.where(other >= 0, 0.5 * (mine + theirs), mine)
            value = jnp.where(live_rows(count, size, slot, face, mine.shape), value, 0.0)
            averaged[slot, face] = value
            vec[face * width : (face + 1) * width] = value.astype(BF16)
        products = multiply(schur, vec, slot, width)
        sent = []
        for face in range(faces):
            value = load[slot, face].astype(F32) - products[face]
            value = jnp.where(live_rows(count, size, slot, face, value.shape), value, 0.0)
            local[slot, face] = value
            if face < 4:
                sent.append(value)
        send_faces((s0, s1, s2, s3), slot, sent)


def scale_slot(slot, values, ids, deluxe, spread_weight, given, scaled, coarse_in):
    partner, count, size = ids
    rows = []
    faces = len(values)
    _, _, width, _ = deluxe.shape
    for face, value in enumerate(values):
        half = value.astype(BF16)
        blocks = [deluxe[slot, face]]
        if face < 4:
            other = jnp.maximum(partner[slot, face], 0)
            blocks.append(from_device(given, face, other * width, width))
        for side, block in enumerate(blocks):
            part = lax.dot_general(
                block, half, (((0,), (0,)), ((), ())), preferred_element_type=F32
            )
            part = jnp.where(live_rows(count, size, slot, face, part.shape), part, 0.0)
            scaled[slot, face + side * faces] = part.astype(BF16)
            if side == 0 and coarse_in is not None:
                rows.append(jnp.sum(spread_weight[slot, face] * part, axis=0, keepdims=True))
    if coarse_in is not None:
        coarse_in[pl.ds(pl.multiple_of(slot * faces, 8), faces)] = jnp.concatenate(rows, axis=0)


def restrict(coarse_map_t, coarse_in):
    count = coarse_map_t.shape[1]
    coarse_in[count:] = jnp.dot(
        coarse_map_t[...], coarse_in[:count], precision=precise, preferred_element_type=F32
    )


def first_scale_kernel(partner, size, count, local, deluxe, spread_weight, coarse_map_t, *refs):
    got, given = refs[:4], refs[4:8]
    residual, scaled, coarse_in = refs[8:]
    slots, faces = local.shape[:2]

    def one_slot(slot, carry):
        values = []
        for face in range(faces):
            other = partner[slot, face]
            theirs = from_face(local, got, jnp.maximum(other, 0), face)
            value = local[slot, face] + jnp.where(other >= 0, theirs, 0.0)
            residual[slot, face] = value
            values.append(value)
        scale_slot(slot, values, (partner, count, size), deluxe, spread_weight, given, scaled, coarse_in)
        return carry

    lax.fori_loop(0, slots, one_slot, 0)
    restrict(coarse_map_t, coarse_in)


def make_next_scale_kernel(layout, halves):
    def next_scale_kernel(partner, size, count, *refs):
        pairs = refs[:halves]
        old_residual, image, deluxe = refs[halves : halves + 3]
        got, given = refs[halves + 3 : halves + 7], refs[halves + 7 : halves + 11]
        residual, full_image, scaled, totals = refs[halves + 11 :]
        slots, faces = image.shape[:2]
        packed = pairs[0].shape[0] // 2
        found = None
        for rows in pairs:
            for start in (layout.far_sums, packed + layout.far_sums):
                part = rows[start : start + 8]
                found = part if found is None else found + part
        totals[...] = found
        step = found[0:1] / found[1:2]

        def one_slot(slot, carry):
            values = []
            for face in range(faces):
                other = partner[slot, face]
                theirs = from_face(image, got, jnp.maximum(other, 0), face).astype(F32)
                full = image[slot, face] + jnp.where(other >= 0, theirs, 0.0)
                full_image[slot, face] = full
                value = old_residual[slot, face] - step * full
                residual[slot, face] = value
                values.append(value)
            scale_slot(slot, values, (partner, count, size), deluxe, None, given, scaled, None)
            return carry

        lax.fori_loop(0, slots, one_slot, 0)

    return next_scale_kernel


def inverse_kernel(partner, scaled, face_inverse, g0, g1, g2, g3, local_part):
    given = (g0, g1, g2, g3)
    slots, faces, width, _ = face_inverse.shape

    def one_slot(slot, carry):
        for face in range(faces + 4):
            if face < faces:
                block = face_inverse[slot, face]
            else:
                other = jnp.maximum(partner[slot, face - faces], 0)
                block = from_device(given, face - faces, (slots + other) * width, width)
            local_part[slot, face] = jnp.dot(
                block, scaled[slot, face], preferred_element_type=F32
            )
        return carry

    lax.fori_loop(0, slots, one_slot, 0)


def vector_kernel(pack, partner, size, count, deluxe, weight, *refs):
    given, packs = refs[:4], refs[4:8]
    spread, vectors = refs[8:]
    slots, faces, width, columns = deluxe.shape
    lanes = lax.broadcasted_iota(jnp.int32, (1, width), 1)

    def vector(block, row, live):
        row = jnp.where(lanes < live, row, 0.0)
        value = jnp.sum(block.astype(F32) * row, axis=1, keepdims=True)
        return jnp.broadcast_to(value, (width, columns))

    for face in range(faces):
        rows = pack.read(packs, face, 0) if face < 4 else None
        for slot in range(slots):
            live = jnp.where(slot < count[0, 0], size[slot, face], 0)
            number = slot * faces + face
            vectors[slot, face] = vector(deluxe[slot, face], weight[number : number + 1], live)
            if face < 4:
                other = partner[slot, face]
                row = jnp.zeros((1, width), F32)
                for place in range(slots):
                    number = place * faces + (face ^ 1)
                    row = jnp.where(other == place, rows[number : number + 1], row)
                spread[slot, face] = jnp.broadcast_to(row, (columns, width)).T
                block = from_device(given, face, jnp.maximum(other, 0) * width, width)
                vectors[slot, faces + face] = vector(block, row, live)


def make_group_kernel(pack, narrow, slots):
    def group_kernel(*refs):
        rows_of = refs[:narrow]
        coarse_group = refs[narrow]
        got = refs[narrow + 1 : narrow + 5]
        packed, group_part, group_vec = refs[narrow + 5 :]
        each = coarse_group.shape[0]
        faces = each // slots
        here = lax.axis_index("narrow")
        restricted = None
        for back, rows in enumerate(rows_of):
            place = (here + narrow - back) % narrow
            group_vec[pl.ds(pl.multiple_of(place * each, 8), each)] = rows[:each]
            part = rows[each:]
            restricted = part if restricted is None else restricted + part
        group = jnp.concatenate(
            [coarse_group[...], pack.read(got, 0, 1), pack.read(got, 1, 1)], axis=0
        )
        part = exact(group, group_vec[...])
        group_part[...] = part
        picked = [
            part[slot * faces + face : slot * faces + face + 1]
            for face in (2, 3)
            for slot in range(slots)
        ]
        quotient, columns = restricted.shape
        filler = packed.shape[0] - quotient - len(picked)
        packed[...] = jnp.concatenate(
            [restricted] + picked + [jnp.zeros((filler, columns), F32)], axis=0
        )

    return group_kernel


class Layout:
    def __init__(self, slots, faces, quotient, narrow):
        self.each = slots * faces
        self.beside = self.each
        self.restricted = -(-(self.each + 4 * slots) // 8) * 8
        self.sums = self.restricted + 3 * quotient
        self.end = self.sums + 8
        self.far_sums = 3 * quotient
        self.far_group = self.far_sums + 8
        self.far_beside = -(-(self.far_group + 2 * slots) // 8) * 8
        self.far_end = -(-(self.far_beside + 2 * narrow * slots) // 8) * 8


def make_next_group_kernel(pack, layout, narrow, slots):
    def next_group_kernel(*refs):
        rows_of = refs[:narrow]
        coarse_group = refs[narrow]
        got = refs[narrow + 1 : narrow + 5]
        packed, group_part, group_vec = refs[narrow + 5 :]
        each = layout.each
        faces = each // slots
        here = lax.axis_index("narrow")
        packed[...] = jnp.zeros(packed.shape, F32)
        carried = None
        for back, rows in enumerate(rows_of):
            place = (here + narrow - back) % narrow
            group_vec[pl.ds(pl.multiple_of(place * each, 8), each)] = rows[:each]
            part = rows[layout.restricted :]
            carried = part if carried is None else carried + part
        packed[: carried.shape[0]] = carried
        for back, rows in enumerate(rows_of):
            place = (here + narrow - back) % narrow
            for slot in range(slots):
                for face, shift in ((0, narrow - 1), (1, 1)):
                    row = layout.beside + face * slots + slot
                    target = (place + shift) % narrow * each + slot * faces + (face ^ 1)
                    group_vec[pl.ds(target, 1)] += rows[row : row + 1]
                for face in (2, 3):
                    row = layout.beside + face * slots + slot
                    target = layout.far_beside + ((face - 2) * narrow + place) * slots + slot
                    packed[pl.ds(target, 1)] = rows[row : row + 1]
        group = jnp.concatenate(
            [coarse_group[...], pack.read(got, 0, 1), pack.read(got, 1, 1)], axis=0
        )
        part = exact(group, group_vec[...])
        group_part[...] = part
        for face in (2, 3):
            for slot in range(slots):
                row = layout.far_group + (face - 2) * slots + slot
                number = slot * faces + face
                packed[row : row + 1] = part[number : number + 1]

    return next_group_kernel


def make_apply_kernel(pack, layout, narrow, halves, later):
    def apply_kernel(partner, size, count, *refs):
        pairs = refs[:halves]
        refs = refs[halves:]
        group_part, map_t, coarse_top, local_part, spread_weight, across_weight, deluxe = refs[:7]
        given, packs = refs[7:11], refs[11:15]
        residual, schur = refs[15:17]
        refs = refs[17:]
        if later:
            old_direction, old_image, coarse_group, totals, old_coarse = refs[:5]
            direction, image, sums, s0, s1, s2, s3 = refs[5:12]
            weighted, everyone, every_pack, coarse_out, vec, beside = refs[12:]
        else:
            vectors = refs[0]
            direction, image, message, coarse_out, s0, s1, s2, s3 = refs[1:9]
            weighted, everyone, every_pack, vec = refs[9:]
        slots, faces, width, columns = direction.shape
        quotient, each = map_t.shape
        here = lax.axis_index("wide")
        wide = 2 * halves
        packed = pairs[0].shape[0] // 2
        far_group = layout.far_group if later else quotient
        for half, rows in enumerate(pairs):
            for other in range(2):
                place = here ^ (2 * half + other)
                every_pack[pl.ds(pl.multiple_of(place * packed, 8), packed)] = rows[
                    other * packed : (other + 1) * packed
                ]
        for place in range(wide):
            start = place * packed
            value = every_pack[start : start + quotient]
            if later:
                above = (place + 1) % wide * packed + quotient
                below = (place + wide - 1) % wide * packed + 2 * quotient
                value = value + every_pack[above : above + quotient]
                value = value + every_pack[below : below + quotient]
            everyone[place * quotient : (place + 1) * quotient] = value
        tops = exact(
            jnp.concatenate(
                [coarse_top[...], pack.read(packs, 2, 3), pack.read(packs, 3, 3)], axis=0
            ),
            everyone[...],
        )
        own_top = tops[:quotient]

        def from_beside(shift, group):
            beside[...] = jnp.zeros(beside.shape, F32)
            for face, side in ((2, wide - 1), (3, 1)):
                source = (here + shift + side) % wide * packed + layout.far_beside
                source = source + (narrow * slots if face == 2 else 0)
                for member in range(narrow):
                    for slot in range(slots):
                        target = member * each + slot * faces + face
                        beside[target : target + 1] = every_pack[
                            pl.ds(source + member * slots + slot, 1)
                        ]
            return exact(group, beside[...])

        own_group = group_part[...]
        if later:
            group = jnp.concatenate(
                [coarse_group[...], pack.read(packs, 0, 1), pack.read(packs, 1, 1)], axis=0
            )
            own_group = own_group + from_beside(0, group)
        coarse_out[:each] = own_group[:each] + exact_t(map_t[...], own_top)
        for face in range(4):
            top = own_top if face < 2 else tops[(face - 1) * quotient : face * quotient]
            value = exact_t(pack.read(packs, face, 2), top)
            start = (face + 1) * each
            if face < 2:
                value = value + own_group[start : start + each]
            elif later:
                shift = wide - 1 if face == 2 else 1
                value = value + from_beside(shift, pack.read(packs, face, 1))
            coarse_out[start : start + each] = value
            if face >= 2:
                side = (here + (wide - 1 if face == 2 else 1)) % wide
                source = side * packed + far_group + (slots if face == 2 else 0)
                for slot in range(slots):
                    row = start + slot * faces + (face ^ 1)
                    coarse_out[row : row + 1] += every_pack[pl.ds(source + slot, 1)]
        if later:
            step = totals[0:1] / totals[1:2]
            coarse_out[...] = old_coarse[...] - step * coarse_out[...]

        def coarse_row(face, other):
            return coarse_out[pl.ds((face + 1) * each + other * faces + (face ^ 1), 1)]

        def weigh(part, weight, row, block, live):
            value = part + weight * row
            value = jnp.where(live, value, 0.0).astype(BF16)
            value = jnp.dot(block, value, preferred_element_type=F32)
            return jnp.where(live, value, 0.0)

        def weigh_slot(slot, carry):
            for face in range(faces):
                live = live_rows(count, size, slot, face, (width, columns))
                weighted[slot, face] = weigh(
                    local_part[slot, face],
                    spread_weight[slot, face],
                    coarse_out[pl.ds(slot * faces + face, 1)],
                    deluxe[slot, face],
                    live,
                )
                if face < 4:
                    other = partner[slot, face]
                    place = jnp.maximum(other, 0)
                    theirs = weigh(
                        local_part[slot, faces + face],
                        across_weight[slot, face],
                        coarse_row(face, place),
                        from_device(given, face, place * width, width),
                        live,
                    )
                    direction[slot, face] = jnp.where(other >= 0, theirs, 0.0)
            return carry

        lax.fori_loop(0, slots, weigh_slot, 0)

        def one_slot(slot, carry):
            norm, curve, cross = carry
            for face in range(faces):
                other = partner[slot, face]
                mine = weighted[slot, face]
                if face < 4:
                    value = mine + direction[slot, face]
                else:
                    theirs = weighted[jnp.maximum(other, 0), face ^ 1]
                    value = mine + jnp.where(other >= 0, theirs, 0.0)
                direction[slot, face] = value
                half = value.astype(BF16)
                rows = slice(face * width, (face + 1) * width)
                vec[rows, :columns] = half
                if later:
                    vec[rows, columns:] = (value - half.astype(F32)).astype(BF16)
                norm = norm + fold(residual[slot, face] * mine)
            products = multiply(schur, vec, slot, width)
            sent = []
            for face in range(faces):
                live = live_rows(count, size, slot, face, (width, columns))
                value = products[face]
                if later:
                    value = value[:, :columns] + value[:, columns:]
                value = jnp.where(live, value, 0.0)
                image[slot, face] = value
                curve = curve + fold(direction[slot, face] * value)
                if later:
                    cross = cross + fold(
                        direction[slot, face] * old_image[slot, face]
                        + old_direction[slot, face] * value
                    )
                if face < 4:
                    sent.append(value)
            send_faces((s0, s1, s2, s3), slot, sent)
            return norm, curve, cross

        zero = jnp.zeros((8, columns), F32)
        found = lax.fori_loop(0, slots, one_slot, (zero, zero, zero))
        rows = [jnp.sum(one, axis=0, keepdims=True) for one in found]
        rows.append(jnp.zeros((5, columns), F32))
        local_sums = jnp.concatenate(rows, axis=0)
        if later:
            sums[...] = local_sums
            return
        message[...] = jnp.zeros(message.shape, F32)
        message[layout.sums : layout.sums + 8] = local_sums

        def coarse_slot(slot, carry):
            rows = []
            blocks = []
            for face in range(faces):
                other = partner[slot, face]
                value = image[slot, face]
                if face >= 4:
                    theirs = image[jnp.maximum(other, 0), face ^ 1]
                    value = value + jnp.where(other >= 0, theirs, 0.0)
                rows.append(jnp.sum(vectors[slot, face] * value, axis=0, keepdims=True))
                if face < 4:
                    row = jnp.sum(vectors[slot, faces + face] * value, axis=0, keepdims=True)
                    blocks += [jnp.where(other == place, row, 0.0) for place in range(slots)]
            message[pl.ds(pl.multiple_of(slot * faces, 8), faces)] = jnp.concatenate(rows, axis=0)
            return carry + jnp.concatenate(blocks, axis=0)

        blocks = lax.fori_loop(0, slots, coarse_slot, jnp.zeros((4 * slots, columns), F32))
        message[layout.beside : layout.beside + 4 * slots] = blocks
        parts = [exact(map_t[...], message[:each])]
        for face in range(4):
            spread = []
            for slot in range(slots):
                before = face ^ 1
                spread.append(jnp.zeros((before, columns), F32)) if before else None
                row = face * slots + slot
                spread.append(blocks[row : row + 1])
                after = faces - 1 - before
                spread.append(jnp.zeros((after, columns), F32))
            value = exact(pack.read(packs, face, 2), jnp.concatenate(spread, axis=0))
            if face < 2:
                parts[0] = parts[0] + value
            else:
                parts.append(value)
        message[layout.restricted : layout.restricted + 3 * quotient] = jnp.concatenate(
            parts, axis=0
        )

    return apply_kernel


def finish_kernel(partner, averaged, direction, precond, residual, full_image, image, first_sums, later_sums, g0, g1, g2, g3, solution_out, residual_out):
    got = (g0, g1, g2, g3)
    slots, faces = image.shape[:2]
    first = first_sums[...]
    later = later_sums[...]
    first_step = first[0:1] / first[1:2]
    ratio = later[0:1] / first[0:1]
    curve = later[1:2] + ratio * (later[2:3] + ratio * first[1:2])
    step = later[0:1] / curve
    old_step = first_step + step * ratio

    def one_slot(slot, carry):
        for face in range(faces):
            other = partner[slot, face]
            theirs = from_face(image, got, jnp.maximum(other, 0), face).astype(F32)
            full = image[slot, face] + jnp.where(other >= 0, theirs, 0.0)
            full = full + ratio * full_image[slot, face]
            residual_out[slot, face] = residual[slot, face] - step * full
            solution_out[slot, face] = (
                averaged[slot, face]
                + old_step * direction[slot, face]
                + step * precond[slot, face]
            )
        return carry

    lax.fori_loop(0, slots, one_slot, 0)


def body(
    schur_matrix,
    face_inverse,
    deluxe,
    primal_weight,
    coarse_group,
    coarse_map,
    coarse_top,
    load_vector,
    previous,
    slot_count,
    partner,
    face_size,
):
    schur_matrix = schur_matrix[0, 0]
    face_inverse = face_inverse[0, 0]
    deluxe = deluxe[0, 0]
    coarse_group = coarse_group[0]
    coarse_map = coarse_map[0]
    load_vector = load_vector[0, 0]
    previous = previous[0, 0]
    partner = partner[0, 0]
    face_size = face_size[0, 0]
    shape = load_vector.shape
    slots, faces, width, columns = shape
    order = schur_matrix.shape[1]
    quotient = coarse_map.shape[1]
    wide = lax.axis_size("wide")
    narrow = lax.axis_size("narrow")
    one_face = (slots * width, columns)
    each = slots * faces
    pack = Pack(
        slots * width,
        columns,
        (each, width),
        coarse_group.shape,
        (quotient, each),
        coarse_top.shape,
    )

    narrow_near = [(i, i ^ 1) for i in range(narrow)]
    narrow_far = [(i, i + 1 if i % 2 else i - 1) for i in range(1, narrow - 1)]
    wide_near = [(i, i ^ 1) for i in range(wide)]
    wide_far = [(i, (i + 1 if i % 2 else i - 1) % wide) for i in range(wide)]

    def swap(sends):
        return (
            lax.ppermute(sends[0], "narrow", narrow_near),
            lax.ppermute(sends[1], "narrow", narrow_far),
            lax.ppermute(sends[2], "wide", wide_near),
            lax.ppermute(sends[3], "wide", wide_far),
        )

    def of_group(rows):
        got = [rows]
        for back in range(1, narrow):
            ring = [(i, (i + back) % narrow) for i in range(narrow)]
            got.append(lax.ppermute(rows, "narrow", ring))
        return got

    def across(rows, step):
        return lax.ppermute(rows, "wide", [(i, i ^ step) for i in range(wide)])

    def spread_rows(rows):
        pair = jnp.concatenate([rows, across(rows, 1)], axis=0)
        return pair, [pair] + [across(pair, step) for step in range(2, wide, 2)]

    def send(*sources):
        rows = len(sources) * slots * width
        return call(send_kernel, (), sources, [((rows, columns), BF16)] * 4)

    got = swap(send(previous))
    given = swap(send(deluxe, face_inverse))
    flat_weight = primal_weight[0, 0].reshape(each, width)
    spread_weight = jnp.broadcast_to(primal_weight[0, 0][..., None], shape)
    coarse_map_t = coarse_map.T
    ids = (partner, face_size, slot_count)
    vec = pltpu.VMEM((order, columns), BF16)
    run_start = functools.partial(
        call,
        functools.partial(start_kernel, pack),
        ids,
        (previous, load_vector, schur_matrix, flat_weight, coarse_group, coarse_map_t, coarse_top)
        + got,
        [(shape, F32), (shape, F32)] + [((pack.end, columns), F32)] * 4,
        [vec],
    )
    averaged, local, *sends = run_start()
    wider = (slots, faces + 4, width, columns)
    scale_outs = [(wider, BF16), ((each + quotient, columns), F32)]
    packed_rows = -(-(quotient + 2 * slots) // 8) * 8
    packs = swap(sends)
    layout = Layout(slots, faces, quotient, narrow)
    across_weight, vectors = call(
        functools.partial(vector_kernel, pack),
        ids,
        (deluxe, flat_weight) + given + packs,
        [((slots, 4, width, columns), F32), (wider, F32)],
    )

    def invert(scaled):
        return call(inverse_kernel, (partner,), (scaled, face_inverse) + given, [(wider, F32)])[0]

    def apply_to(later, pairs, group_part, local_part, more, outs, send_type, scratch):
        packed = pairs[0].shape[0] // 2
        return call(
            make_apply_kernel(pack, layout, narrow, wide // 2, later),
            ids,
            (
                *pairs,
                group_part,
                coarse_map_t,
                coarse_top,
                local_part,
                spread_weight,
                across_weight,
                deluxe,
            )
            + given
            + packs
            + more,
            [(shape, F32), (shape, F32)] + outs + [(one_face, send_type)] * 4,
            [
                pltpu.VMEM(shape, F32),
                pltpu.VMEM((wide * quotient, columns), F32),
                pltpu.VMEM((wide * packed, columns), F32),
            ]
            + scratch,
        )

    residual, scaled, coarse_in = call(
        first_scale_kernel,
        ids,
        (local, deluxe, spread_weight, coarse_map_t) + packs + given,
        [(shape, F32)] + scale_outs,
    )
    group_outs = [((3 * each, columns), F32)]
    group_scratch = [pltpu.VMEM((narrow * each, columns), F32)]
    packed, group_part = call(
        make_group_kernel(pack, narrow, slots),
        (),
        (*of_group(coarse_in), coarse_group) + packs,
        [((packed_rows, columns), F32)] + group_outs,
        group_scratch,
    )
    pair, pairs = spread_rows(packed)
    direction, image, message, coarse_out, *sends = apply_to(
        False,
        pairs,
        group_part,
        invert(scaled),
        (residual, schur_matrix, vectors),
        [((layout.end, columns), F32), ((5 * each, columns), F32)],
        F32,
        [vec],
    )
    rows_of = of_group(message)
    got = swap(sends)
    packed, group_part = call(
        make_next_group_kernel(pack, layout, narrow, slots),
        (),
        (*rows_of, coarse_group) + packs,
        [((layout.far_end, columns), F32)] + group_outs,
        group_scratch,
    )
    pair = jnp.concatenate([packed, across(packed, 1)], axis=0)
    pairs = [pair] + [across(pair, step) for step in range(2, wide, 2)]
    residual, full_image, scaled, first_sums = call(
        make_next_scale_kernel(layout, wide // 2),
        ids,
        (*pairs, residual, image, deluxe) + got + given,
        [(shape, F32), (shape, F32), (wider, BF16), ((8, columns), F32)],
    )
    precond, later_image, later_sums, *sends = apply_to(
        True,
        pairs,
        group_part,
        invert(scaled),
        (residual, schur_matrix, direction, image, coarse_group, first_sums, coarse_out),
        [((8, columns), F32)],
        BF16,
        [
            pltpu.VMEM((5 * each, columns), F32),
            pltpu.VMEM((order, 2 * columns), BF16),
            pltpu.VMEM((narrow * each, columns), F32),
        ],
    )
    later_sums = sum(of_group(later_sums))
    got = swap(sends)
    later_sums = later_sums + across(later_sums, 1)
    later_sums = sum([later_sums] + [across(later_sums, step) for step in range(2, wide, 2)])
    solution, residual = call(
        finish_kernel,
        (partner,),
        (averaged, direction, precond, residual, full_image, later_image, first_sums, later_sums)
        + got,
        [(shape, F32), (shape, F32)],
    )
    return (solution[None, None], residual[None, None])


def solution(mesh):
    in_specs = (
        P("wide", "narrow", None, None, None),
        P("wide", "narrow", None, None, None, None),
        P("wide", "narrow", None, None, None, None),
        P("wide", "narrow", None, None, None),
        P("wide", "narrow", None),
        P("wide", "narrow", None),
        P("wide", None),
        P("wide", "narrow", None, None, None, None),
        P("wide", "narrow", None, None, None, None),
        P("wide", "narrow"),
        P("wide", "narrow", None, None),
        P("wide", "narrow", None, None),
    )
    out_specs = (
        P("wide", "narrow", None, None, None, None),
        P("wide", "narrow", None, None, None, None),
    )
    return jax.shard_map(body, mesh=mesh, in_specs=in_specs, out_specs=out_specs, check_vma=False)
```
